8 devices in a mesh: dp: 2 (over z, y), tp: 4 (over x, core).
Axes of the slice: x: 2, y: 2, z: 1, core: 2. Of those that a mesh axis runs over, the one named last changes fastest.
Arguments:
- tokens: int32 [64], P('dp'), parts along dimension 0
- positions: int32 [64], P('dp'), parts along dimension 0
- self_keys: bfloat16 [2, 64, 448, 12, 64], P(None, 'dp', None, 'tp'), parts along dimension 1
- self_vals: bfloat16 [2, 64, 448, 12, 64], P(None, 'dp', None, 'tp'), parts along dimension 1
- cross_keys: bfloat16 [2, 64, 1500, 12, 64], P(None, 'dp', None, 'tp'), parts along dimension 1
- cross_vals: bfloat16 [2, 64, 1500, 12, 64], P(None, 'dp', None, 'tp'), parts along dimension 1
- embed_table: bfloat16 [52224, 768], P('tp')
- pos_table: bfloat16 [448, 768], replicated
- w_qkv: bfloat16 [2, 768, 3, 12, 64], P(None, None, None, 'tp')
- w_cq: bfloat16 [2, 768, 12, 64], P(None, None, 'tp')
- in_bias: float32 [2, 3, 12, 64], P(None, None, 'tp')
- w_out: bfloat16 [2, 2, 12, 64, 768], P(None, None, 'tp')
- out_bias: float32 [2, 3, 768], replicated
- w_fc1: bfloat16 [2, 768, 3072], P(None, None, 'tp')
- b_fc1: float32 [2, 3072], P(None, 'tp')
- w_fc2: bfloat16 [2, 3072, 768], P(None, 'tp')
- ln_layers: float32 [2, 3, 2, 768], replicated
- ln_final: float32 [2, 768], replicated
Outputs:
- output 1: float32 [64, 52224], P('dp', 'tp'), parts along dimension 0
- output 2: bfloat16 [2, 64, 448, 12, 64], P(None, 'dp', None, 'tp'), parts along dimension 1
- output 3: bfloat16 [2, 64, 448, 12, 64], P(None, 'dp', None, 'tp'), parts along dimension 1
There are 2 independent parts. The reference program is written for one: setup_inputs(seed, part) draws one part's arguments, and reference() takes and returns one part's arrays. A program takes and returns all parts, laid end to end along the dimension named above; an argument that names none is the same for every part.
All inputs are finite; a program needn't handle non-finite values.
Results may differ from the reference program's by a relative error of at most 0.0121347.
Values are sent between devices in bfloat16 or wider.
A program may use at most 1 GiB of HBM per device.

```python
import jax
import jax.numpy as jnp
from jax import lax

SEQ_BATCH = 32
D_MODEL = 768
N_HEADS = 12
HEAD_DIM = 64
FF_DIM = 3072
VOCAB_SIZE = 51864
VOCAB_PAD = 52224
TEXT_CTX = 448
FRAMES = 1500
LAYERS = 2
FRAME_RANK = 8


def setup_inputs(seed: int = 0, part: int = 0) -> dict:
    base_key = jax.random.key(seed)
    part_keys = jax.random.split(jax.random.fold_in(base_key, part), 12)
    shared_keys = jax.random.split(jax.random.fold_in(base_key, 1000003), 14)

    def normal_draw(key_in, draw_shape, factor):
        return jax.random.normal(key_in, draw_shape, jnp.float32) * factor

    def structured(code_key, basis_key, noise_key, length, factor, noise_std):
        frame_codes = normal_draw(code_key, (SEQ_BATCH, length, FRAME_RANK), 1.0)
        code_basis = normal_draw(basis_key, (LAYERS, SEQ_BATCH, FRAME_RANK, N_HEADS, HEAD_DIM), factor * FRAME_RANK ** -0.5)
        mixed_rows = jnp.einsum('btr,lbrhe->lbthe', frame_codes, code_basis)
        return mixed_rows + normal_draw(noise_key, (LAYERS, SEQ_BATCH, length, N_HEADS, HEAD_DIM), noise_std)

    tokens = jax.random.randint(part_keys[0], (SEQ_BATCH,), 0, VOCAB_SIZE, dtype=jnp.int32)
    tokens = tokens.at[0].set(VOCAB_SIZE - 1).at[1].set(0)
    positions = jax.random.randint(part_keys[1], (SEQ_BATCH,), 0, TEXT_CTX, dtype=jnp.int32)
    positions = positions.at[0].set(TEXT_CTX - 1).at[1].set(0)
    self_keys = structured(part_keys[2], part_keys[3], part_keys[4], TEXT_CTX, 1.0, 0.3).astype(jnp.bfloat16)
    self_vals = structured(part_keys[2], part_keys[5], part_keys[6], TEXT_CTX, 1.0, 0.5).astype(jnp.bfloat16)
    cross_keys = structured(part_keys[7], part_keys[8], part_keys[9], FRAMES, 1.0, 0.3).astype(jnp.bfloat16)
    cross_vals = structured(part_keys[7], part_keys[10], part_keys[11], FRAMES, 1.0, 0.5).astype(jnp.bfloat16)
    embed_table = normal_draw(shared_keys[12], (VOCAB_PAD, D_MODEL), D_MODEL ** -0.25).astype(jnp.bfloat16)
    pos_table = normal_draw(shared_keys[13], (TEXT_CTX, D_MODEL), 0.5).astype(jnp.bfloat16)
    w_qkv = normal_draw(shared_keys[0], (LAYERS, D_MODEL, 3, N_HEADS, HEAD_DIM), D_MODEL ** -0.5).astype(jnp.bfloat16)
    w_cq = normal_draw(shared_keys[1], (LAYERS, D_MODEL, N_HEADS, HEAD_DIM), D_MODEL ** -0.5).astype(jnp.bfloat16)
    in_bias = normal_draw(shared_keys[2], (LAYERS, 3, N_HEADS, HEAD_DIM), 0.3)
    w_out = normal_draw(shared_keys[3], (LAYERS, 2, N_HEADS, HEAD_DIM, D_MODEL), D_MODEL ** -0.5).astype(jnp.bfloat16)
    out_bias = normal_draw(shared_keys[4], (LAYERS, 3, D_MODEL), 0.3)
    w_fc1 = normal_draw(shared_keys[5], (LAYERS, D_MODEL, FF_DIM), D_MODEL ** -0.5).astype(jnp.bfloat16)
    b_fc1 = normal_draw(shared_keys[6], (LAYERS, FF_DIM), 0.3)
    w_fc2 = normal_draw(shared_keys[7], (LAYERS, FF_DIM, D_MODEL), FF_DIM ** -0.5).astype(jnp.bfloat16)
    ln_layers = jnp.concatenate([1.0 + normal_draw(shared_keys[8], (LAYERS, 3, 1, D_MODEL), 0.2), normal_draw(shared_keys[9], (LAYERS, 3, 1, D_MODEL), 0.2)], axis=2)
    ln_final = jnp.concatenate([1.0 + normal_draw(shared_keys[10], (1, D_MODEL), 0.2), normal_draw(shared_keys[11], (1, D_MODEL), 0.2)], axis=0)
    return {'tokens': tokens, 'positions': positions, 'self_keys': self_keys, 'self_vals': self_vals, 'cross_keys': cross_keys, 'cross_vals': cross_vals, 'embed_table': embed_table, 'pos_table': pos_table, 'w_qkv': w_qkv, 'w_cq': w_cq, 'in_bias': in_bias, 'w_out': w_out, 'out_bias': out_bias, 'w_fc1': w_fc1, 'b_fc1': b_fc1, 'w_fc2': w_fc2, 'ln_layers': ln_layers, 'ln_final': ln_final}


def layer_norm(resid_in, ln_gain, ln_shift):
    row_mean = jnp.mean(resid_in, axis=-1, keepdims=True)
    centred = resid_in - row_mean
    variance = jnp.mean(centred * centred, axis=-1, keepdims=True)
    return (centred * lax.rsqrt(variance + 1e-5) * ln_gain + ln_shift).astype(jnp.bfloat16)


def attend(queries, key_rows, val_rows, mask_add):
    scores = jnp.einsum('bhe,bthe->bht', queries.astype(jnp.float32), key_rows.astype(jnp.float32)) * (HEAD_DIM ** -0.5) + mask_add
    weights = jax.nn.softmax(scores, axis=-1).astype(jnp.bfloat16)
    mixed_vals = jnp.einsum('bht,bthe->bhe', weights.astype(jnp.float32), val_rows.astype(jnp.float32))
    return mixed_vals.astype(jnp.bfloat16)


def project_out(attended, out_weight):
    summed = jnp.einsum('bhe,hed->bd', attended.astype(jnp.float32), out_weight.astype(jnp.float32))
    return summed.astype(jnp.bfloat16).astype(jnp.float32)


def reference(tokens, positions, self_keys, self_vals, cross_keys, cross_vals, embed_table, pos_table, w_qkv, w_cq, in_bias, w_out, out_bias, w_fc1, b_fc1, w_fc2, ln_layers, ln_final):
    residual = embed_table[tokens].astype(jnp.float32) + pos_table[positions].astype(jnp.float32)
    cache_pos = jnp.arange(TEXT_CTX)[None, :]
    write_mask = (cache_pos == positions[:, None])[:, :, None, None]
    self_mask = jnp.where(cache_pos <= positions[:, None], 0.0, -1e30)[:, None, :]

    def layer_body(resid_in, layer_args):
        (cache_keys, cache_vals, frame_keys, frame_vals, qkv_weight, cq_weight, bias_in, out_weight, bias_out, fc1_weight, fc1_bias, fc2_weight, ln_params) = layer_args
        hidden = layer_norm(resid_in, ln_params[0, 0], ln_params[0, 1])
        projected = jnp.einsum('bd,dthe->bthe', hidden.astype(jnp.float32), qkv_weight.astype(jnp.float32))
        queries = (projected[:, 0] + bias_in[0]).astype(jnp.bfloat16)
        key_new = projected[:, 1].astype(jnp.bfloat16)
        val_new = (projected[:, 2] + bias_in[1]).astype(jnp.bfloat16)
        keys_now = jnp.where(write_mask, key_new[:, None], cache_keys)
        vals_now = jnp.where(write_mask, val_new[:, None], cache_vals)
        resid_mid = resid_in + project_out(attend(queries, keys_now, vals_now, self_mask), out_weight[0]) + bias_out[0]
        hidden = layer_norm(resid_mid, ln_params[1, 0], ln_params[1, 1])
        cross_q = (jnp.einsum('bd,dhe->bhe', hidden.astype(jnp.float32), cq_weight.astype(jnp.float32)) + bias_in[2]).astype(jnp.bfloat16)
        resid_mid = resid_mid + project_out(attend(cross_q, frame_keys, frame_vals, 0.0), out_weight[1]) + bias_out[1]
        hidden = layer_norm(resid_mid, ln_params[2, 0], ln_params[2, 1])
        fc1_out = jnp.dot(hidden, fc1_weight, preferred_element_type=jnp.float32) + fc1_bias
        active = jax.nn.gelu(fc1_out, approximate=False).astype(jnp.bfloat16)
        fc2_out = jnp.dot(active, fc2_weight, preferred_element_type=jnp.float32).astype(jnp.bfloat16).astype(jnp.float32)
        resid_out = resid_mid + fc2_out + bias_out[2]
        return resid_out, (keys_now, vals_now)

    residual, new_caches = lax.scan(layer_body, residual, (self_keys, self_vals, cross_keys, cross_vals, w_qkv, w_cq, in_bias, w_out, out_bias, w_fc1, b_fc1, w_fc2, ln_layers))
    final_hidden = layer_norm(residual, ln_final[0], ln_final[1])
    logits = jnp.dot(final_hidden, embed_table.T, preferred_element_type=jnp.float32)
    return logits, new_caches[0], new_caches[1]
```

```python
import jax
import jax.numpy as jnp
from jax import lax
from jax.experimental import pallas as pl
from jax.experimental.pallas import tpu as pltpu
from jax.sharding import PartitionSpec as P

F32 = jnp.float32
BF16 = jnp.bfloat16
MESH = pl.DeviceIdType.MESH
ANY = pl.ANY

SLOTS = 19
UNROLL = 4
SELF_CHUNK = 8
VOCAB_CHUNK = 768
STAGE_SEQS = 4
STAGE_SLOTS = 8
MIB = 1024 * 1024


def layer_norm(residual, ln_gain, ln_shift):
    row_mean = jnp.mean(residual, axis=-1, keepdims=True)
    centred = residual - row_mean
    variance = jnp.mean(centred * centred, axis=-1, keepdims=True)
    return (centred * lax.rsqrt(variance + 1e-5) * ln_gain + ln_shift).astype(BF16)


def dot_nn(left, right):
    return lax.dot_general(left, right, (((1,), (0,)), ((), ())), preferred_element_type=F32)


def dot_nt(left, right):
    return lax.dot_general(left, right, (((1,), (1,)), ((), ())), preferred_element_type=F32)


def gather_kernel(tok_s, pos_s, embed_h, ptab_h, emb_o, pos_o, ebuf, pbuf, rows, esem, psem):
    n_seq = rows.shape[1]
    shard_rows = embed_h.shape[0]
    first = lax.axis_index('tp') * shard_rows

    def local_row(b):
        local = tok_s[b] - first
        owned = (local >= 0) & (local < shard_rows)
        return jnp.where(owned, local, 0), owned

    def e_copy(b):
        row, _ = local_row(b)
        base = pl.multiple_of((row // 16) * 16, 16)
        return pltpu.make_async_copy(embed_h.at[pl.ds(base, 16)], ebuf.at[b], esem.at[b])

    def p_copy(b):
        base = pl.multiple_of((pos_s[b] // 16) * 16, 16)
        return pltpu.make_async_copy(ptab_h.at[pl.ds(base, 16)], pbuf.at[b], psem.at[b])

    def start(b, carry):
        e_copy(b).start()
        p_copy(b).start()
        return carry

    lax.fori_loop(0, n_seq, start, 0)
    sub = lax.broadcasted_iota(jnp.int32, (16, embed_h.shape[1]), 0)

    def pick(b, carry):
        row, owned = local_row(b)
        e_copy(b).wait()
        p_copy(b).wait()
        want = jnp.where(owned, row % 16, -1)
        rows[0, pl.ds(b, 1), :] = jnp.sum(jnp.where(sub == want, ebuf[b].astype(F32), 0.0), axis=0, keepdims=True)
        rows[1, pl.ds(b, 1), :] = jnp.sum(jnp.where(sub == pos_s[b] % 16, pbuf[b].astype(F32), 0.0), axis=0, keepdims=True)
        return carry

    lax.fori_loop(0, n_seq, pick, 0)
    emb_o[...] = rows[0].astype(BF16)
    pos_o[...] = rows[1]


def layers_kernel(pos_s, picked, prow, inb, outb, lnp, bf1, lnf, wqkv_h, wcq_h, wout_h, w1_h, w2_h, sk_h, sv_h, ck_h, cv_h,
                  xo, kn, vn, skv,
                  x, q, o, ring, wqkv, wcq, wout, w1, w2, emb, ar, sem_w, sem_s, sem_c, sem_es, sem_er, sem_as, sem_ar):
    n_layer, n_seq, width = kn.shape
    half = n_seq // 2
    n_items = n_layer * n_seq
    n_chunk = n_seq // SELF_CHUNK
    me = lax.axis_index('tp')
    peers = [lax.rem(me + d, 4) for d in (1, 2, 3)]

    weights = ((wqkv_h, wqkv), (wcq_h, wcq), (wout_h, wout), (w1_h, w1), (w2_h, w2))

    def w_copy(i, layer):
        return pltpu.make_async_copy(weights[i][0].at[layer], weights[i][1].at[layer], sem_w.at[i, layer])

    def s_copy(kv, layer, c):
        rows = pl.ds(c * SELF_CHUNK, SELF_CHUNK)
        return pltpu.make_async_copy((sk_h, sv_h)[kv].at[layer, rows], skv.at[kv, layer, rows], sem_s.at[kv, layer, c])

    def c_copy(kv, item):
        slot = lax.rem(item, SLOTS)
        return pltpu.make_async_copy((ck_h, cv_h)[kv].at[lax.div(item, n_seq), lax.rem(item, n_seq)], ring.at[slot, kv], sem_c.at[kv, slot])

    def start_item(item):
        c_copy(0, item).start()
        c_copy(1, item).start()

    w_copy(0, 0).start()
    for c in range(n_chunk):
        s_copy(0, 0, c).start()
        s_copy(1, 0, c).start()
    w_copy(2, 0).start()
    w_copy(1, 0).start()
    for item in range(SLOTS):
        start_item(jnp.int32(item))
        if item == SLOTS // 2:
            w_copy(3, 0).start()
            w_copy(4, 0).start()
    for layer in range(1, n_layer):
        w_copy(0, layer).start()
        for c in range(n_chunk):
            s_copy(0, layer, c).start()
            s_copy(1, layer, c).start()
        for i in (2, 1, 3, 4):
            w_copy(i, layer).start()

    barrier = pltpu.get_barrier_semaphore()
    for peer in peers:
        pl.semaphore_signal(barrier, inc=1, device_id={'tp': peer}, device_id_type=MESH)
    pl.semaphore_wait(barrier, 3)

    def e_copy(d):
        return pltpu.make_async_remote_copy(picked, emb.at[me], sem_es.at[d], sem_er.at[d], device_id={'tp': peers[d]}, device_id_type=MESH)

    for d in range(3):
        e_copy(d).start()
    emb[me] = picked[...]
    for d in range(3):
        e_copy(d).wait()
    x[...] = (emb[0].astype(F32) + emb[1].astype(F32) + emb[2].astype(F32) + emb[3].astype(F32)) + prow[...]

    head_mask = lax.broadcasted_iota(jnp.int32, (8, width), 0) == lax.div(lax.broadcasted_iota(jnp.int32, (8, width), 1), 64)

    def a_copy(inst, d):
        return pltpu.make_async_remote_copy(ar.at[inst, me], ar.at[inst, me], sem_as.at[inst, d], sem_ar.at[inst, d], device_id={'tp': peers[d]}, device_id_type=MESH)

    def send(inst, part):
        ar[inst, me] = part
        for d in range(3):
            a_copy(inst, d).start()

    def receive(inst, rows, bias):
        for d in range(3):
            a_copy(inst, d).wait()
        total = (ar[inst, 0] + ar[inst, 1]) + (ar[inst, 2] + ar[inst, 3])
        x[rows, :] = (x[rows, :] + total.astype(BF16).astype(F32)) + bias

    def in_bias_row(kind, layer):
        return jnp.concatenate([inb[kind, h, pl.ds(layer, 1), :] for h in range(3)], axis=1)

    def query_block(b):
        return jnp.where(head_mask, q[pl.ds(b, 1), :] * 0.125, 0.0)

    def fold_heads(mixed):
        return jnp.sum(jnp.where(head_mask, mixed, 0.0), axis=0, keepdims=True)

    def self_stage(layer, hf):
        rows = pl.ds(hf * half, half)
        hidden = layer_norm(x[rows, :], lnp[layer, 0, 0:1, :], lnp[layer, 0, 1:2, :])
        if hf == 0:
            w_copy(0, layer).wait()
        round32 = lambda z: z.astype(BF16).astype(F32)
        q[rows, :] = round32(dot_nt(hidden, wqkv[layer, 0:width, :]) + in_bias_row(0, layer))
        kn[layer, rows, :] = round32(dot_nt(hidden, wqkv[layer, width:2 * width, :]))
        vn[layer, rows, :] = round32(dot_nt(hidden, wqkv[layer, 2 * width:3 * width, :]) + in_bias_row(1, layer))
        lane = lax.broadcasted_iota(jnp.int32, (8, skv.shape[4]), 1)

        def body(g, carry):
            seqs = [g * UNROLL + u for u in range(UNROLL)]
            blocks = [query_block(b) for b in seqs]
            scores = [dot_nn(blocks[u].astype(BF16), skv[0, layer, seqs[u]]) for u in range(UNROLL)]
            wts = []
            for u, b in enumerate(seqs):
                past = lane < pos_s[b]
                s = jnp.where(past, scores[u], -1e30)
                s_new = jnp.sum(blocks[u] * kn[layer, pl.ds(b, 1), :], axis=1, keepdims=True)
                peak = jnp.maximum(jnp.max(s, axis=1, keepdims=True), s_new)
                e = jnp.where(past, jnp.exp(s - peak), 0.0)
                e_new = jnp.exp(s_new - peak)
                inv = 1.0 / (jnp.sum(e, axis=1, keepdims=True) + e_new)
                wts.append(((e * inv).astype(BF16), (e_new * inv).astype(BF16).astype(F32)))
            for u, b in enumerate(seqs):
                mixed = dot_nt(wts[u][0], skv[1, layer, b]) + wts[u][1] * vn[layer, pl.ds(b, 1), :]
                o[pl.ds(b, 1), :] = fold_heads(mixed)
            return carry

        per = SELF_CHUNK // UNROLL
        for c in range(hf * half // SELF_CHUNK, (hf + 1) * half // SELF_CHUNK):
            s_copy(0, layer, c).wait()
            s_copy(1, layer, c).wait()
            lax.fori_loop(c * per, (c + 1) * per, body, 0)
        if hf == 0:
            w_copy(2, layer).wait()
        send((layer * 3 + 0) * 2 + hf, dot_nn(o[rows, :].astype(BF16), wout[layer, 0]))

    def cross_stage(layer, hf):
        rows = pl.ds(hf * half, half)
        hidden = layer_norm(x[rows, :], lnp[layer, 1, 0:1, :], lnp[layer, 1, 1:2, :])
        if hf == 0:
            w_copy(1, layer).wait()
        q[rows, :] = (dot_nt(hidden, wcq[layer]) + in_bias_row(2, layer)).astype(BF16).astype(F32)

        def body(g, carry):
            seqs = [g * UNROLL + u for u in range(UNROLL)]
            items = [layer * n_seq + b for b in seqs]
            slots = [lax.rem(item, SLOTS) for item in items]
            for item in items:
                c_copy(0, item).wait()
                c_copy(1, item).wait()
            scores = [dot_nn(query_block(seqs[u]).astype(BF16), ring[slots[u], 0]) for u in range(UNROLL)]
            wts = []
            for u in range(UNROLL):
                e = jnp.exp(scores[u] - jnp.max(scores[u], axis=1, keepdims=True))
                inv = 1.0 / jnp.sum(e, axis=1, keepdims=True)
                wts.append((e * inv).astype(BF16))
            for u, b in enumerate(seqs):
                o[pl.ds(b, 1), :] = fold_heads(dot_nt(wts[u], ring[slots[u], 1]))
            for item in items:
                @pl.when(item + SLOTS < n_items)
                def _():
                    start_item(item + SLOTS)
            return carry

        lax.fori_loop(hf * half // UNROLL, (hf + 1) * half // UNROLL, body, 0)
        send((layer * 3 + 1) * 2 + hf, dot_nn(o[rows, :].astype(BF16), wout[layer, 1]))

    def mlp_stage(layer, hf):
        rows = pl.ds(hf * half, half)
        hidden = layer_norm(x[rows, :], lnp[layer, 2, 0:1, :], lnp[layer, 2, 1:2, :])
        if hf == 0:
            w_copy(3, layer).wait()
            w_copy(4, layer).wait()
        pre = dot_nn(hidden, w1[layer]) + bf1[pl.ds(layer, 1), :]
        active = (0.5 * pre * (1.0 + lax.erf(pre * (0.5 ** 0.5)))).astype(BF16)
        send((layer * 3 + 2) * 2 + hf, dot_nn(active, w2[layer]))

    stages = (self_stage, cross_stage, mlp_stage)
    for step in range(n_layer * 3 + 1):
        layer, kind = divmod(step, 3)
        for hf in range(2):
            rows = pl.ds(hf * half, half)
            if step:
                prev_layer, prev_kind = divmod(step - 1, 3)
                receive((step - 1) * 2 + hf, rows, outb[prev_kind, prev_layer:prev_layer + 1, :])
            if step < n_layer * 3:
                stages[kind](layer, hf)
    xo[...] = layer_norm(x[...], lnf[0:1, :], lnf[1:2, :])


def tail_kernel(pos_s, xf, kn, vn, skv, embed_h, logit_h, nk_h, nv_h, ebuf, lbuf, stage, newt, sem_e, sem_l, sem_n):
    _, n_layer, n_seq, width, ctx = skv.shape
    n_vocab = ebuf.shape[0]
    n_chunk = n_seq // STAGE_SEQS

    def e_copy(c):
        return pltpu.make_async_copy(embed_h.at[pl.ds(pl.multiple_of(c * VOCAB_CHUNK, VOCAB_CHUNK), VOCAB_CHUNK)], ebuf.at[c], sem_e.at[c])

    def l_copy(c):
        return pltpu.make_async_copy(lbuf.at[c], logit_h.at[:, pl.ds(pl.multiple_of(c * VOCAB_CHUNK, VOCAB_CHUNK), VOCAB_CHUNK)], sem_l.at[c])

    for c in range(n_vocab):
        e_copy(c).start()

    lane = lax.broadcasted_iota(jnp.int32, (width, ctx), 1)
    col = lax.broadcasted_iota(jnp.int32, (width, n_seq), 1)

    for kv, (new, out_h) in enumerate(((kn, nk_h), (vn, nv_h))):
        for layer in range(n_layer):
            newt[...] = new[layer].T
            first = (kv * n_layer + layer) * n_chunk

            def n_copy(c, out_h=out_h, layer=layer, first=first):
                slot = lax.rem(c + first, STAGE_SLOTS)
                return pltpu.make_async_copy(stage.at[slot], out_h.at[layer, pl.ds(c * STAGE_SEQS, STAGE_SEQS)], sem_n.at[slot])

            def body(c, carry, kv=kv, layer=layer, first=first, n_copy=n_copy):
                @pl.when(c + first >= STAGE_SLOTS)
                def _():
                    n_copy(c).wait()
                slot = lax.rem(c + first, STAGE_SLOTS)
                for s in range(STAGE_SEQS):
                    b = c * STAGE_SEQS + s
                    column = jnp.sum(jnp.where(col == b, newt[...], 0.0), axis=1, keepdims=True)
                    stage[slot, s] = jnp.where(lane == pos_s[b], column, skv[kv, layer, b].astype(F32)).astype(BF16)
                n_copy(c).start()
                return carry

            lax.fori_loop(0, n_chunk, body, 0)

    def logit_body(c, carry):
        e_copy(c).wait()
        lbuf[c] = dot_nt(xf[...], ebuf[c])
        l_copy(c).start()
        return carry

    lax.fori_loop(0, n_vocab, logit_body, 0)

    def drain(c, carry):
        l_copy(c).wait()
        return carry

    lax.fori_loop(0, n_vocab, drain, 0)
    for slot in range(STAGE_SLOTS):
        pltpu.make_async_copy(stage.at[slot], nv_h.at[0, pl.ds(0, STAGE_SEQS)], sem_n.at[slot]).wait()


def solution(mesh):
    smem = pl.BlockSpec(memory_space=pltpu.SMEM)
    vmem = pl.BlockSpec(memory_space=pltpu.VMEM)
    hbm = pl.BlockSpec(memory_space=ANY)
    dma = pltpu.SemaphoreType.DMA
    on_chip = lambda z: pltpu.with_memory_space_constraint(z, pltpu.VMEM)

    def local_step(tokens, positions, self_keys, self_vals, cross_keys, cross_vals, embed_table, pos_table, w_qkv, w_cq, in_bias, w_out, out_bias, w_fc1, b_fc1, w_fc2, ln_layers, ln_final):
        n_layer, n_seq, ctx, n_head, head_dim = self_keys.shape
        frames = cross_keys.shape[2]
        width = n_head * head_dim
        model = embed_table.shape[1]
        hidden_units = w_fc1.shape[2]
        vocab_rows = embed_table.shape[0]
        n_vocab = vocab_rows // VOCAB_CHUNK
        flat = lambda cache: jnp.transpose(cache, (0, 1, 3, 4, 2)).reshape(n_layer, n_seq, width, cache.shape[2])
        sk, sv, ck, cv = flat(self_keys), flat(self_vals), flat(cross_keys), flat(cross_vals)

        picked, prow = pl.pallas_call(
            gather_kernel,
            out_shape=(pltpu.VMEM((n_seq, model), BF16), pltpu.VMEM((n_seq, model), F32)),
            in_specs=[smem, smem, hbm, hbm],
            out_specs=(vmem, vmem),
            scratch_shapes=[
                pltpu.VMEM((n_seq, 16, model), BF16), pltpu.VMEM((n_seq, 16, model), BF16), pltpu.VMEM((2, n_seq, model), F32),
                dma((n_seq,)), dma((n_seq,)),
            ],
            name='gather_rows',
        )(tokens, positions, embed_table, pos_table)

        wqkv = jnp.transpose(w_qkv, (0, 2, 3, 4, 1)).reshape(n_layer, 3 * width, model)
        wcq = jnp.transpose(w_cq, (0, 2, 3, 1)).reshape(n_layer, width, model)
        wout = w_out.reshape(n_layer, 2, width, model)
        n_inst = n_layer * 3 * 2
        xf, kn, vn, skv = pl.pallas_call(
            layers_kernel,
            out_shape=(
                pltpu.VMEM((n_seq, model), BF16),
                pltpu.VMEM((n_layer, n_seq, width), F32),
                pltpu.VMEM((n_layer, n_seq, width), F32),
                pltpu.VMEM((2,) + sk.shape, BF16),
            ),
            in_specs=[smem] + [vmem] * 7 + [hbm] * 9,
            out_specs=(vmem, vmem, vmem, vmem),
            scratch_shapes=[
                pltpu.VMEM((n_seq, model), F32), pltpu.VMEM((n_seq, width), F32), pltpu.VMEM((n_seq, width), F32),
                pltpu.VMEM((SLOTS, 2, width, frames), BF16),
                pltpu.VMEM(wqkv.shape, BF16), pltpu.VMEM(wcq.shape, BF16), pltpu.VMEM(wout.shape, BF16),
                pltpu.VMEM(w_fc1.shape, BF16), pltpu.VMEM(w_fc2.shape, BF16),
                pltpu.VMEM((4, n_seq, model), BF16), pltpu.VMEM((n_inst, 4, n_seq // 2, model), F32),
                dma((5, n_layer)), dma((2, n_layer, n_seq // SELF_CHUNK)), dma((2, SLOTS)), dma((3,)), dma((3,)), dma((n_inst, 3)), dma((n_inst, 3)),
            ],
            compiler_params=pltpu.CompilerParams(collective_id=0, has_side_effects=True, vmem_limit_bytes=37 * MIB),
            name='decoder_layers',
        )(positions, on_chip(picked), on_chip(prow), jnp.transpose(in_bias, (1, 2, 0, 3)), jnp.transpose(out_bias, (1, 0, 2)), ln_layers, b_fc1, ln_final,
          wqkv, wcq, wout, w_fc1, w_fc2, sk, sv, ck, cv)

        logits, nk, nv = pl.pallas_call(
            tail_kernel,
            out_shape=(
                jax.ShapeDtypeStruct((n_seq, vocab_rows), F32),
                jax.ShapeDtypeStruct(sk.shape, BF16),
                jax.ShapeDtypeStruct(sv.shape, BF16),
            ),
            in_specs=[smem, vmem, vmem, vmem, vmem, hbm],
            out_specs=(hbm, hbm, hbm),
            scratch_shapes=[
                pltpu.VMEM((n_vocab, VOCAB_CHUNK, model), BF16), pltpu.VMEM((n_vocab, n_seq, VOCAB_CHUNK), F32),
                pltpu.VMEM((STAGE_SLOTS, STAGE_SEQS, width, ctx), BF16), pltpu.VMEM((width, n_seq), F32),
                dma((n_vocab,)), dma((n_vocab,)), dma((STAGE_SLOTS,)),
            ],
            compiler_params=pltpu.CompilerParams(vmem_limit_bytes=34 * MIB),
            name='logits_and_caches',
        )(positions, *(on_chip(z) for z in (xf, kn, vn, skv)), embed_table)
        unflat = lambda cache: jnp.transpose(cache.reshape(n_layer, n_seq, n_head, head_dim, ctx), (0, 1, 4, 2, 3))
        return logits, unflat(nk), unflat(nv)

    batch_spec = P('dp')
    cache_spec = P(None, 'dp', None, 'tp', None)
    in_specs = (batch_spec, batch_spec, cache_spec, cache_spec, cache_spec, cache_spec, P('tp', None), P(None, None), P(None, None, None, 'tp', None), P(None, None, 'tp', None), P(None, None, 'tp', None), P(None, None, 'tp', None, None), P(None, None, None), P(None, None, 'tp'), P(None, 'tp'), P(None, 'tp', None), P(None, None, None, None), P(None, None))
    out_specs = (P('dp', 'tp'), cache_spec, cache_spec)
    return jax.shard_map(local_step, mesh=mesh, in_specs=in_specs, out_specs=out_specs, check_vma=False)
```

```python
import jax
import jax.numpy as jnp
from jax import lax
from jax.experimental import pallas as pl
from jax.experimental.pallas import tpu as pltpu
from jax.sharding import PartitionSpec as P

F32 = jnp.float32
BF16 = jnp.bfloat16
MESH = pl.DeviceIdType.MESH
ANY = pl.ANY

SLOTS = 5
GROUP = 4
PARTS = 2
BLOCK = 2
VOCAB_AHEAD = 5
LOGIT_LAG = 2
VOCAB_CHUNK = 768
STAGE_SLOTS = 8
MIB = 1024 * 1024


def layer_norm(residual, ln_gain, ln_shift):
    row_mean = jnp.mean(residual, axis=-1, keepdims=True)
    centred = residual - row_mean
    variance = jnp.mean(centred * centred, axis=-1, keepdims=True)
    return (centred * lax.rsqrt(variance + 1e-5) * ln_gain + ln_shift).astype(BF16)


def dot_nn(left, right):
    return lax.dot_general(left, right, (((1,), (0,)), ((), ())), preferred_element_type=F32)


def dot_nt(left, right):
    return lax.dot_general(left, right, (((1,), (1,)), ((), ())), preferred_element_type=F32)


def gather_kernel(tok_s, embed_h, emb_o, ebuf, rows, esem):
    n_seq = rows.shape[0]
    shard_rows = embed_h.shape[0]
    first = lax.axis_index('tp') * shard_rows

    def local_row(b):
        local = tok_s[b] - first
        owned = (local >= 0) & (local < shard_rows)
        return jnp.where(owned, local, 0), owned

    def e_copy(b):
        row, _ = local_row(b)
        base = pl.multiple_of((row // 16) * 16, 16)
        return pltpu.make_async_copy(embed_h.at[pl.ds(base, 16)], ebuf.at[b], esem.at[b])

    for b in range(n_seq):
        e_copy(b).start()
    sub = lax.broadcasted_iota(jnp.int32, (16, embed_h.shape[1]), 0)
    for b in range(n_seq):
        row, owned = local_row(b)
        e_copy(b).wait()
        want = jnp.where(owned, row % 16, -1)
        rows[b:b + 1, :] = jnp.sum(jnp.where(sub == want, ebuf[b].astype(F32), 0.0), axis=0, keepdims=True)
    emb_o[...] = rows[...].astype(BF16)


def layers_kernel(pos_s, picked, inb, outb, lnp, bf1, lnf, ptab_h, wqkv_h, wcq_h, wout_h, w1_h, w2_h, sk_h, sv_h, ck_h, cv_h,
                  xo, kn, vn, skv,
                  x, of, hot, ptab, ring, wqkv, wcq, wout, w1, w2, emb, ar, sem_p, sem_w, sem_s, sem_c, sem_es, sem_er, sem_as, sem_ar):
    n_layer, n_seq, width = kn.shape
    per_part = n_seq // PARTS
    n_group = per_part // GROUP
    layer_items = PARTS * n_group
    n_items = n_layer * layer_items
    stacked = GROUP * width
    frames = ring.shape[-1]
    ctx = skv.shape[-1]
    me = lax.axis_index('tp')
    peers = [lax.rem(me + d, 4) for d in (1, 2, 3)]

    weights = ((wqkv_h, wqkv), (wcq_h, wcq), (wout_h, wout), (w1_h, w1), (w2_h, w2))

    def w_copy(i, layer):
        return pltpu.make_async_copy(weights[i][0].at[layer], weights[i][1].at[layer], sem_w.at[i, layer])

    def s_copy(kv, layer, item):
        part, g = divmod(item, n_group)
        return pltpu.make_async_copy((sk_h, sv_h)[kv].at[layer, part, :, g], skv.at[kv, layer, item], sem_s.at[kv, layer, item])

    def c_copy(kv, item):
        slot = item % SLOTS
        layer, rest = divmod(item, layer_items)
        part, g = divmod(rest, n_group)
        return pltpu.make_async_copy((ck_h, cv_h)[kv].at[layer, part, :, g], ring.at[kv, slot], sem_c.at[kv, slot])

    def start_self(layer, part):
        for item in range(part * n_group, (part + 1) * n_group):
            s_copy(0, layer, item).start()
            s_copy(1, layer, item).start()

    def start_weights(layer, which):
        for i in which:
            w_copy(i, layer).start()

    def start_cross(items):
        for item in items:
            if item < n_items:
                c_copy(0, item).start()
                c_copy(1, item).start()

    tab_copy = pltpu.make_async_copy(ptab_h, ptab, sem_p.at[0])
    tab_copy.start()
    start_weights(0, (0,))
    for part in range(PARTS):
        start_self(0, part)
        start_weights(0, ((2,), (1,))[part])

    barrier = pltpu.get_barrier_semaphore()
    for peer in peers:
        pl.semaphore_signal(barrier, inc=1, device_id={'tp': peer}, device_id_type=MESH)
    pl.semaphore_wait(barrier, 3)
    start_cross((0,))

    def e_copy(d):
        return pltpu.make_async_remote_copy(picked, emb.at[me], sem_es.at[d], sem_er.at[d], device_id={'tp': peers[d]}, device_id_type=MESH)

    for d in range(3):
        e_copy(d).start()
    emb[me] = picked[...]
    tab_lane = lax.broadcasted_iota(jnp.int32, (1, ptab.shape[0]), 1)
    for b in range(n_seq):
        hot[b:b + 1, :] = jnp.where(tab_lane == pos_s[b], 1.0, 0.0)
    tab_copy.wait()
    x[...] = dot_nn(hot[...].astype(BF16), ptab[...])
    for d in range(3):
        e_copy(d).wait()
    x[...] = (emb[0].astype(F32) + emb[1].astype(F32) + emb[2].astype(F32) + emb[3].astype(F32)) + x[...]
    start_cross((1, 2))

    lane_block = lax.div(lax.broadcasted_iota(jnp.int32, (16, stacked), 1), 64)
    block_mask = lax.broadcasted_iota(jnp.int32, (16, stacked), 0) == lane_block
    row_seq = lax.div(lax.broadcasted_iota(jnp.int32, (16, 1), 0), width // 64)
    lane = lax.broadcasted_iota(jnp.int32, (16, ctx), 1)

    def a_copy(inst, d):
        return pltpu.make_async_remote_copy(ar.at[inst, me], ar.at[inst, me], sem_as.at[inst, d], sem_ar.at[inst, d], device_id={'tp': peers[d]}, device_id_type=MESH)

    def send(inst, value):
        ar[inst, me] = value
        for d in range(3):
            a_copy(inst, d).start()

    def receive(inst, rows, bias):
        for d in range(3):
            a_copy(inst, d).wait()
        total = (ar[inst, 0] + ar[inst, 1]) + (ar[inst, 2] + ar[inst, 3])
        x[rows, :] = (x[rows, :] + total.astype(BF16).astype(F32)) + bias

    def in_bias_row(kind, layer):
        return jnp.concatenate([inb[kind, h, layer:layer + 1, :] for h in range(3)], axis=1)

    def stack(rows):
        return jnp.concatenate([rows[u * n_group:(u + 1) * n_group] for u in range(GROUP)], axis=1)

    def query_blocks(flat):
        return [jnp.where(block_mask, flat[g:g + 1] * 0.125, 0.0) for g in range(n_group)]

    def fold(mixed):
        return jnp.sum(jnp.where(block_mask, mixed, 0.0), axis=0, keepdims=True)

    def attended():
        return jnp.concatenate([of[:, u * width:(u + 1) * width] for u in range(GROUP)], axis=0).astype(BF16)

    def round32(z):
        return z.astype(BF16).astype(F32)

    def self_stage(layer, part, rows):
        hidden = layer_norm(x[rows, :], lnp[layer, 0, 0:1, :], lnp[layer, 0, 1:2, :])

        if part == 0:
            w_copy(0, layer).wait()
            w_copy(2, layer).wait()

        q = round32(dot_nt(hidden, wqkv[layer, 0:width, :]) + in_bias_row(0, layer))
        k_new = round32(dot_nt(hidden, wqkv[layer, width:2 * width, :]))
        v_new = round32(dot_nt(hidden, wqkv[layer, 2 * width:3 * width, :]) + in_bias_row(1, layer))
        kn[layer, rows, :] = k_new
        vn[layer, rows, :] = v_new
        k_flat, v_flat = stack(k_new), stack(v_new)
        items = [part * n_group + g for g in range(n_group)]
        for item in items:
            s_copy(0, layer, item).wait()
            s_copy(1, layer, item).wait()
        blocks = query_blocks(stack(q))
        scores = [dot_nn(blocks[g].astype(BF16), skv[0, layer, items[g]].reshape(stacked, ctx)) for g in range(n_group)]
        mixed = []
        for g in range(n_group):
            limit = jnp.full((16, 1), 0, jnp.int32)
            for u in range(GROUP):
                limit = jnp.where(row_seq == u, pos_s[part * per_part + u * n_group + g], limit)
            past = lane < limit
            s = jnp.where(past, scores[g], -1e30)
            s_new = jnp.sum(blocks[g] * k_flat[g:g + 1], axis=1, keepdims=True)
            peak = jnp.maximum(jnp.max(s, axis=1, keepdims=True), s_new)
            e = jnp.where(past, jnp.exp(s - peak), 0.0)
            e_new = jnp.exp(s_new - peak)
            inv = 1.0 / (jnp.sum(e, axis=1, keepdims=True) + e_new)
            w_new = round32(e_new * inv)
            mixed.append(dot_nt((e * inv).astype(BF16), skv[1, layer, items[g]].reshape(stacked, ctx)) + w_new * v_flat[g:g + 1])
        for g in range(n_group):
            of[g:g + 1, :] = fold(mixed[g])
        return dot_nn(attended(), wout[layer, 0])

    def cross_stage(layer, part, rows):
        hidden = layer_norm(x[rows, :], lnp[layer, 1, 0:1, :], lnp[layer, 1, 1:2, :])

        if part == 0:
            w_copy(1, layer).wait()

        q = round32(dot_nt(hidden, wcq[layer]) + in_bias_row(2, layer))
        blocks = query_blocks(stack(q))
        items = [(layer * PARTS + part) * n_group + g for g in range(n_group)]
        mixed = []
        for first in range(0, n_group, BLOCK):
            block = range(first, first + BLOCK)
            for g in block:
                c_copy(0, items[g]).wait()
                c_copy(1, items[g]).wait()
            scores = [dot_nn(blocks[g].astype(BF16), ring[0, items[g] % SLOTS].reshape(stacked, frames)) for g in block]
            for g in block:
                s = scores[g - first]
                e = jnp.exp(s - jnp.max(s, axis=1, keepdims=True))
                inv = 1.0 / jnp.sum(e, axis=1, keepdims=True)
                mixed.append(dot_nt((e * inv).astype(BF16), ring[1, items[g] % SLOTS].reshape(stacked, frames)))
            for g in block:
                of[g:g + 1, :] = fold(mixed[g])
            start_cross([items[g] + SLOTS for g in block])
        heads = attended()
        return dot_nn(heads, wout[layer, 1])

    def mlp_stage(layer, part, rows):
        hidden = layer_norm(x[rows, :], lnp[layer, 2, 0:1, :], lnp[layer, 2, 1:2, :])

        if part == 0:
            w_copy(3, layer).wait()
            w_copy(4, layer).wait()

        pre = dot_nn(hidden, w1[layer]) + bf1[layer:layer + 1, :]
        active = (0.5 * pre * (1.0 + lax.erf(pre * (0.5 ** 0.5)))).astype(BF16)
        return dot_nn(active, w2[layer])

    stages = (self_stage, cross_stage, mlp_stage)
    def start_ahead(layer, kind, part):
        if kind == 0 and layer == 0:
            if part == 0:
                start_cross((3,))
            else:
                start_cross((4,))
                start_weights(0, (3, 4))
        if layer + 1 < n_layer:
            if kind == 1:
                if part == 0:
                    start_weights(layer + 1, (0,))
                start_self(layer + 1, part)
                start_weights(layer + 1, ((2,), (1,))[part])
            if kind == 2 and part == 0:
                start_weights(layer + 1, (3, 4))

    for step in range(n_layer * 3 + 1):
        for part in range(PARTS):
            rows = pl.ds(part * per_part, per_part)
            if step:
                prev_layer, prev_kind = divmod(step - 1, 3)
                receive((step - 1) * PARTS + part, rows, outb[prev_kind, prev_layer:prev_layer + 1, :])
            if step < n_layer * 3:
                layer, kind = divmod(step, 3)
                send(step * PARTS + part, stages[kind](layer, part, rows))
                start_ahead(layer, kind, part)
    xo[...] = layer_norm(x[...], lnf[0:1, :], lnf[1:2, :])


def tail_kernel(pos_s, xf, kn, vn, skv, embed_h, logit_h, nk_h, nv_h, ebuf, lbuf, stage, newt, sem_e, sem_l, sem_n):
    _, n_layer, n_chunk, _, width, ctx = skv.shape
    n_seq = n_chunk * GROUP
    n_group = n_chunk // PARTS
    n_vocab = lbuf.shape[0]
    n_write = 2 * n_layer * n_chunk

    def e_copy(c):
        return pltpu.make_async_copy(embed_h.at[pl.ds(c * VOCAB_CHUNK, VOCAB_CHUNK)], ebuf.at[c], sem_e.at[c])

    def l_copy(c):
        return pltpu.make_async_copy(lbuf.at[c], logit_h.at[:, pl.ds(c * VOCAB_CHUNK, VOCAB_CHUNK)], sem_l.at[c])

    def n_copy(i):
        kv, layer, c = i // (n_layer * n_chunk), i // n_chunk % n_layer, i % n_chunk
        return pltpu.make_async_copy(stage.at[i % STAGE_SLOTS], (nk_h, nv_h)[kv].at[layer, c // n_group, :, c % n_group], sem_n.at[i % STAGE_SLOTS])

    lane = lax.broadcasted_iota(jnp.int32, (16, ctx), 1)

    def write(i):
        kv, layer, c = i // (n_layer * n_chunk), i // n_chunk % n_layer, i % n_chunk
        if c == 0:
            newt[...] = (kn, vn)[kv][layer].T
        if i >= STAGE_SLOTS:
            n_copy(i - STAGE_SLOTS).wait()
        for s in range(GROUP):
            b = (c // n_group * GROUP + s) * n_group + c % n_group
            here = lane == pos_s[b]
            for r in range(0, width, 16):
                column = jnp.broadcast_to(newt[r:r + 16, b:b + 1], (16, ctx)).astype(BF16)
                stage[i % STAGE_SLOTS, s, r:r + 16, :] = jnp.where(here, column, skv[kv, layer, c, s, r:r + 16, :])
        n_copy(i).start()

    def logit(c):
        e_copy(c).wait()
        lbuf[c] = dot_nt(xf[...], ebuf[c])
        l_copy(c).start()

    done = 0
    for c in range(VOCAB_AHEAD):
        e_copy(c).start()
    for i in range(n_write):
        write(i)
        if i % 2 and i // 2 + VOCAB_AHEAD < n_vocab:
            e_copy(i // 2 + VOCAB_AHEAD).start()
        if i >= LOGIT_LAG and i % 2 == 0:
            logit(done)
            done += 1
    for c in range(done, n_vocab):
        logit(c)
    for c in range(n_vocab):
        l_copy(c).wait()
    for i in range(n_write - STAGE_SLOTS, n_write):
        n_copy(i).wait()


def solution(mesh):
    smem = pl.BlockSpec(memory_space=pltpu.SMEM)
    vmem = pl.BlockSpec(memory_space=pltpu.VMEM)
    hbm = pl.BlockSpec(memory_space=ANY)
    dma = pltpu.SemaphoreType.DMA
    on_chip = lambda z: pltpu.with_memory_space_constraint(z, pltpu.VMEM)

    def local_step(tokens, positions, self_keys, self_vals, cross_keys, cross_vals, embed_table, pos_table, w_qkv, w_cq, in_bias, w_out, out_bias, w_fc1, b_fc1, w_fc2, ln_layers, ln_final):
        n_layer, n_seq, ctx, n_head, head_dim = self_keys.shape
        frames = cross_keys.shape[2]
        width = n_head * head_dim
        model = embed_table.shape[1]
        hidden_units = w_fc1.shape[2]
        vocab_rows = embed_table.shape[0]
        n_vocab = vocab_rows // VOCAB_CHUNK
        n_group = n_seq // (PARTS * GROUP)
        flat = lambda cache: jnp.transpose(cache, (0, 1, 3, 4, 2)).reshape(n_layer, PARTS, GROUP, n_group, width, cache.shape[2])
        sk, sv, ck, cv = flat(self_keys), flat(self_vals), flat(cross_keys), flat(cross_vals)

        picked = pl.pallas_call(
            gather_kernel,
            out_shape=pltpu.VMEM((n_seq, model), BF16),
            in_specs=[smem, hbm],
            out_specs=vmem,
            scratch_shapes=[pltpu.VMEM((n_seq, 16, model), BF16), pltpu.VMEM((n_seq, model), F32), dma((n_seq,))],
            name='gather_rows',
        )(tokens, embed_table)

        wqkv = jnp.transpose(w_qkv, (0, 2, 3, 4, 1)).reshape(n_layer, 3 * width, model)
        wcq = jnp.transpose(w_cq, (0, 2, 3, 1)).reshape(n_layer, width, model)
        wout = w_out.reshape(n_layer, 2, width, model)
        n_inst = n_layer * 3 * PARTS
        n_item = PARTS * n_group
        xf, kn, vn, skv = pl.pallas_call(
            layers_kernel,
            out_shape=(
                pltpu.VMEM((n_seq, model), BF16),
                pltpu.VMEM((n_layer, n_seq, width), F32),
                pltpu.VMEM((n_layer, n_seq, width), F32),
                pltpu.VMEM((2, n_layer, n_item, GROUP, width, ctx), BF16),
            ),
            in_specs=[smem] + [vmem] * 6 + [hbm] * 10,
            out_specs=(vmem, vmem, vmem, vmem),
            scratch_shapes=[
                pltpu.VMEM((n_seq, model), F32), pltpu.VMEM((n_group, GROUP * width), F32),
                pltpu.VMEM((n_seq, ctx), F32), pltpu.VMEM(pos_table.shape, BF16),
                pltpu.VMEM((2, SLOTS, GROUP, width, frames), BF16),
                pltpu.VMEM(wqkv.shape, BF16), pltpu.VMEM(wcq.shape, BF16), pltpu.VMEM(wout.shape, BF16),
                pltpu.VMEM(w_fc1.shape, BF16), pltpu.VMEM(w_fc2.shape, BF16),
                pltpu.VMEM((4, n_seq, model), BF16), pltpu.VMEM((n_inst, 4, n_seq // PARTS, model), F32),
                dma((1,)), dma((5, n_layer)), dma((2, n_layer, n_item)), dma((2, SLOTS)), dma((3,)), dma((3,)), dma((n_inst, 3)), dma((n_inst, 3)),
            ],
            compiler_params=pltpu.CompilerParams(collective_id=0, has_side_effects=True, vmem_limit_bytes=37 * MIB),
            name='decoder_layers',
        )(positions, on_chip(picked), jnp.transpose(in_bias, (1, 2, 0, 3)), jnp.transpose(out_bias, (1, 0, 2)), ln_layers, b_fc1, ln_final,
          pos_table, wqkv, wcq, wout, w_fc1, w_fc2, sk, sv, ck, cv)

        logits, nk, nv = pl.pallas_call(
            tail_kernel,
            out_shape=(
                jax.ShapeDtypeStruct((n_seq, vocab_rows), F32),
                jax.ShapeDtypeStruct(sk.shape, BF16),
                jax.ShapeDtypeStruct(sv.shape, BF16),
            ),
            in_specs=[smem, vmem, vmem, vmem, vmem, hbm],
            out_specs=(hbm, hbm, hbm),
            scratch_shapes=[
                pltpu.VMEM((n_vocab, VOCAB_CHUNK, model), BF16), pltpu.VMEM((n_vocab, n_seq, VOCAB_CHUNK), F32),
                pltpu.VMEM((STAGE_SLOTS, GROUP, width, ctx), BF16), pltpu.VMEM((width, n_seq), F32),
                dma((n_vocab,)), dma((n_vocab,)), dma((STAGE_SLOTS,)),
            ],
            compiler_params=pltpu.CompilerParams(vmem_limit_bytes=34 * MIB),
            name='logits_and_caches',
        )(positions, *(on_chip(z) for z in (xf, kn, vn, skv)), embed_table)
        unflat = lambda cache: jnp.transpose(cache.reshape(n_layer, n_seq, n_head, head_dim, ctx), (0, 1, 4, 2, 3))
        return logits, unflat(nk), unflat(nv)

    batch_spec = P('dp')
    cache_spec = P(None, 'dp', None, 'tp', None)
    in_specs = (batch_spec, batch_spec, cache_spec, cache_spec, cache_spec, cache_spec, P('tp', None), P(None, None), P(None, None, None, 'tp', None), P(None, None, 'tp', None), P(None, None, 'tp', None), P(None, None, 'tp', None, None), P(None, None, None), P(None, None, 'tp'), P(None, 'tp'), P(None, 'tp', None), P(None, None, None, None), P(None, None))
    out_specs = (P('dp', 'tp'), cache_spec, cache_spec)
    return jax.shard_map(local_step, mesh=mesh, in_specs=in_specs, out_specs=out_specs, check_vma=False)
```

```python
import jax
import jax.numpy as jnp
from jax import lax
from jax.experimental import pallas as pl
from jax.experimental.pallas import tpu as pltpu
from jax.sharding import PartitionSpec as P

F32 = jnp.float32
BF16 = jnp.bfloat16
MESH = pl.DeviceIdType.MESH
ANY = pl.ANY

SLOTS = 5
GROUP = 4
PARTS = 2
BLOCK = 2
VOCAB_CHUNK = 768
STAGE_SLOTS = 8
MIB = 1024 * 1024


def layer_norm(residual, ln_gain, ln_shift):
    row_mean = jnp.mean(residual, axis=-1, keepdims=True)
    centred = residual - row_mean
    variance = jnp.mean(centred * centred, axis=-1, keepdims=True)
    return (centred * lax.rsqrt(variance + 1e-5) * ln_gain + ln_shift).astype(BF16)


def dot_nn(left, right):
    return lax.dot_general(left, right, (((1,), (0,)), ((), ())), preferred_element_type=F32)


def dot_nt(left, right):
    return lax.dot_general(left, right, (((1,), (1,)), ((), ())), preferred_element_type=F32)


def chunk_place(c, n_items):
    return c % 2, (n_items + c // 2 % SLOTS) % SLOTS


def gather_kernel(tok_s, embed_h, emb_o, ebuf, rows, esem):
    n_seq = rows.shape[0]
    shard_rows = embed_h.shape[0]
    first = lax.axis_index('tp') * shard_rows

    def local_row(b):
        local = tok_s[b] - first
        owned = (local >= 0) & (local < shard_rows)
        return jnp.where(owned, local, 0), owned

    def e_copy(b):
        row, _ = local_row(b)
        base = pl.multiple_of((row // 16) * 16, 16)
        return pltpu.make_async_copy(embed_h.at[pl.ds(base, 16)], ebuf.at[b], esem.at[b])

    for b in range(n_seq):
        e_copy(b).start()
    sub = lax.broadcasted_iota(jnp.int32, (16, embed_h.shape[1]), 0)
    for b in range(n_seq):
        row, owned = local_row(b)
        e_copy(b).wait()
        want = jnp.where(owned, row % 16, -1)
        rows[b:b + 1, :] = jnp.sum(jnp.where(sub == want, ebuf[b].astype(F32), 0.0), axis=0, keepdims=True)
    emb_o[...] = rows[...].astype(BF16)


def layers_kernel(pos_s, picked, inb, outb, lnp, bf1, lnf, ptab_h, wqkv_h, wcq_h, wout_h, w1_h, w2_h, sk_h, sv_h, ck_h, cv_h, embed_h,
                  xo, kn, vn, ext, ring, skv,
                  x, of, hot, ptab, wqkv, wcq, wout, w1, w2, emb, ar, sem_p, sem_w, sem_s, sem_c, sem_v, sem_es, sem_er, sem_as, sem_ar):
    n_layer, n_seq, width = kn.shape
    per_part = n_seq // PARTS
    n_group = per_part // GROUP
    layer_items = PARTS * n_group
    n_items = n_layer * layer_items
    stacked = GROUP * width
    frames = ring.shape[-1]
    ctx = skv.shape[-1]
    me = lax.axis_index('tp')
    peers = [lax.rem(me + d, 4) for d in (1, 2, 3)]

    weights = ((wqkv_h, wqkv), (wcq_h, wcq), (wout_h, wout), (w1_h, w1), (w2_h, w2))

    def w_copy(i, layer):
        return pltpu.make_async_copy(weights[i][0].at[layer], weights[i][1].at[layer], sem_w.at[i, layer])

    def s_copy(kv, layer, item):
        part, g = divmod(item, n_group)
        return pltpu.make_async_copy((sk_h, sv_h)[kv].at[layer, part, :, g], skv.at[kv, layer, item], sem_s.at[kv, layer, item])

    def c_copy(kv, item):
        slot = item % SLOTS
        layer, rest = divmod(item, layer_items)
        part, g = divmod(rest, n_group)
        return pltpu.make_async_copy((ck_h, cv_h)[kv].at[layer, part, :, g], ring.at[kv, slot], sem_c.at[kv, slot])

    def start_self(layer, part):
        for item in range(part * n_group, (part + 1) * n_group):
            s_copy(0, layer, item).start()
            s_copy(1, layer, item).start()

    def start_weights(layer, which):
        for i in which:
            w_copy(i, layer).start()

    ahead = 2 * SLOTS
    n_extra = ext.shape[0]
    model = embed_h.shape[3]
    split = model - ext.shape[3]

    def v_copies(c):
        kv, slot = chunk_place(c, n_items)
        if c < ahead:
            return [pltpu.make_async_copy(embed_h.at[c], ring.at[kv, slot, :, :, pl.ds(0, model)], sem_v.at[c])]
        return [
            pltpu.make_async_copy(embed_h.at[c, :, :, pl.ds(0, split)], ring.at[kv, slot, :, :, pl.ds(model, split)], sem_v.at[c]),
            pltpu.make_async_copy(embed_h.at[c, :, :, pl.ds(split, model - split)], ext.at[c - ahead], sem_v.at[c + n_extra]),
        ]

    def start_cross(items):
        for item in items:
            for kv in range(2):
                if item < n_items:
                    c_copy(kv, item).start()
                else:
                    c = (item - n_items) * 2 + kv
                    for chunk in (c, c + ahead):
                        if chunk < ahead + n_extra:
                            for copy in v_copies(chunk):
                                copy.start()

    tab_copy = pltpu.make_async_copy(ptab_h, ptab, sem_p.at[0])
    tab_copy.start()
    start_weights(0, (0,))
    for part in range(PARTS):
        start_self(0, part)
        start_weights(0, ((2,), (1,))[part])

    barrier = pltpu.get_barrier_semaphore()
    for peer in peers:
        pl.semaphore_signal(barrier, inc=1, device_id={'tp': peer}, device_id_type=MESH)
    pl.semaphore_wait(barrier, 3)
    start_cross((0, 1))

    def e_copy(d):
        return pltpu.make_async_remote_copy(picked, emb.at[me], sem_es.at[d], sem_er.at[d], device_id={'tp': peers[d]}, device_id_type=MESH)

    for d in range(3):
        e_copy(d).start()
    emb[me] = picked[...]
    tab_lane = lax.broadcasted_iota(jnp.int32, (1, ptab.shape[0]), 1)
    for b in range(n_seq):
        hot[b:b + 1, :] = jnp.where(tab_lane == pos_s[b], 1.0, 0.0)
    tab_copy.wait()
    x[...] = dot_nn(hot[...].astype(BF16), ptab[...])
    for d in range(3):
        e_copy(d).wait()
    x[...] = (emb[0].astype(F32) + emb[1].astype(F32) + emb[2].astype(F32) + emb[3].astype(F32)) + x[...]
    start_cross((2, 3, 4))

    lane_block = lax.div(lax.broadcasted_iota(jnp.int32, (16, stacked), 1), 64)
    block_mask = lax.broadcasted_iota(jnp.int32, (16, stacked), 0) == lane_block
    row_seq = lax.div(lax.broadcasted_iota(jnp.int32, (16, 1), 0), width // 64)
    lane = lax.broadcasted_iota(jnp.int32, (16, ctx), 1)

    def a_copy(inst, d):
        return pltpu.make_async_remote_copy(ar.at[inst, me], ar.at[inst, me], sem_as.at[inst, d], sem_ar.at[inst, d], device_id={'tp': peers[d]}, device_id_type=MESH)

    def send(inst, value):
        ar[inst, me] = value
        for d in range(3):
            a_copy(inst, d).start()

    def receive(inst, rows, bias):
        for d in range(3):
            a_copy(inst, d).wait_recv()
        total = (ar[inst, 0] + ar[inst, 1]) + (ar[inst, 2] + ar[inst, 3])
        x[rows, :] = (x[rows, :] + total.astype(BF16).astype(F32)) + bias

    def in_bias_row(kind, layer):
        return jnp.concatenate([inb[kind, h, layer:layer + 1, :] for h in range(3)], axis=1)

    def stack(rows):
        return jnp.concatenate([rows[u * n_group:(u + 1) * n_group] for u in range(GROUP)], axis=1)

    def query_blocks(flat):
        return [jnp.where(block_mask, flat[g:g + 1] * 0.125, 0.0) for g in range(n_group)]

    def fold(mixed):
        return jnp.sum(jnp.where(block_mask, mixed, 0.0), axis=0, keepdims=True)

    def attended():
        return jnp.concatenate([of[:, u * width:(u + 1) * width] for u in range(GROUP)], axis=0).astype(BF16)

    def round32(z):
        return z.astype(BF16).astype(F32)

    def self_stage(layer, part, rows):
        hidden = layer_norm(x[rows, :], lnp[layer, 0, 0:1, :], lnp[layer, 0, 1:2, :])

        if part == 0:
            w_copy(0, layer).wait()
            w_copy(2, layer).wait()

        q = round32(dot_nt(hidden, wqkv[layer, 0:width, :]) + in_bias_row(0, layer))
        k_new = round32(dot_nt(hidden, wqkv[layer, width:2 * width, :]))
        v_new = round32(dot_nt(hidden, wqkv[layer, 2 * width:3 * width, :]) + in_bias_row(1, layer))
        kn[layer, rows, :] = k_new
        vn[layer, rows, :] = v_new
        k_flat, v_flat = stack(k_new), stack(v_new)
        items = [part * n_group + g for g in range(n_group)]
        for item in items:
            s_copy(0, layer, item).wait()
            s_copy(1, layer, item).wait()
        blocks = query_blocks(stack(q))
        scores = [dot_nn(blocks[g].astype(BF16), skv[0, layer, items[g]].reshape(stacked, ctx)) for g in range(n_group)]
        mixed = []
        for g in range(n_group):
            limit = jnp.full((16, 1), 0, jnp.int32)
            for u in range(GROUP):
                limit = jnp.where(row_seq == u, pos_s[part * per_part + u * n_group + g], limit)
            past = lane < limit
            s = jnp.where(past, scores[g], -1e30)
            s_new = jnp.sum(blocks[g] * k_flat[g:g + 1], axis=1, keepdims=True)
            peak = jnp.maximum(jnp.max(s, axis=1, keepdims=True), s_new)
            e = jnp.where(past, jnp.exp(s - peak), 0.0)
            e_new = jnp.exp(s_new - peak)
            inv = 1.0 / (jnp.sum(e, axis=1, keepdims=True) + e_new)
            w_new = round32(e_new * inv)
            mixed.append(dot_nt((e * inv).astype(BF16), skv[1, layer, items[g]].reshape(stacked, ctx)) + w_new * v_flat[g:g + 1])
        for g in range(n_group):
            of[g:g + 1, :] = fold(mixed[g])
        return dot_nn(attended(), wout[layer, 0])

    def cross_stage(layer, part, rows):
        hidden = layer_norm(x[rows, :], lnp[layer, 1, 0:1, :], lnp[layer, 1, 1:2, :])

        if part == 0:
            w_copy(1, layer).wait()

        q = round32(dot_nt(hidden, wcq[layer]) + in_bias_row(2, layer))
        blocks = query_blocks(stack(q))
        items = [(layer * PARTS + part) * n_group + g for g in range(n_group)]
        mixed = []
        for first in range(0, n_group, BLOCK):
            block = range(first, first + BLOCK)
            for g in block:
                c_copy(0, items[g]).wait()
                c_copy(1, items[g]).wait()
            scores = [dot_nn(blocks[g].astype(BF16), ring[0, items[g] % SLOTS].reshape(stacked, frames)) for g in block]
            for g in block:
                s = scores[g - first]
                e = jnp.exp(s - jnp.max(s, axis=1, keepdims=True))
                inv = 1.0 / jnp.sum(e, axis=1, keepdims=True)
                mixed.append(dot_nt((e * inv).astype(BF16), ring[1, items[g] % SLOTS].reshape(stacked, frames)))
            for g in block:
                of[g:g + 1, :] = fold(mixed[g])
            start_cross([items[g] + SLOTS for g in block])
        heads = attended()
        return dot_nn(heads, wout[layer, 1])

    def mlp_stage(layer, part, rows):
        hidden = layer_norm(x[rows, :], lnp[layer, 2, 0:1, :], lnp[layer, 2, 1:2, :])

        if part == 0:
            w_copy(3, layer).wait()
            w_copy(4, layer).wait()

        pre = dot_nn(hidden, w1[layer]) + bf1[layer:layer + 1, :]
        active = (0.5 * pre * (1.0 + lax.erf(pre * (0.5 ** 0.5)))).astype(BF16)
        return dot_nn(active, w2[layer])

    stages = (self_stage, cross_stage, mlp_stage)
    def start_ahead(layer, kind, part):
        if kind == 0 and layer == 0:
            if part:
                start_weights(0, (3, 4))
        if layer + 1 < n_layer:
            if kind == 1:
                if part == 0:
                    start_weights(layer + 1, (0,))
                start_self(layer + 1, part)
                start_weights(layer + 1, ((2,), (1,))[part])
            if kind == 2 and part == 0:
                start_weights(layer + 1, (3, 4))

    for step in range(n_layer * 3 + 1):
        for part in range(PARTS):
            rows = pl.ds(part * per_part, per_part)
            if step:
                prev_layer, prev_kind = divmod(step - 1, 3)
                receive((step - 1) * PARTS + part, rows, outb[prev_kind, prev_layer:prev_layer + 1, :])
            if step < n_layer * 3:
                layer, kind = divmod(step, 3)
                send(step * PARTS + part, stages[kind](layer, part, rows))
                start_ahead(layer, kind, part)
    xo[...] = layer_norm(x[...], lnf[0:1, :], lnf[1:2, :])
    for inst in range(n_layer * 3 * PARTS):
        for d in range(3):
            a_copy(inst, d).wait_send()
    for c in range(ahead + n_extra):
        for copy in v_copies(c):
            copy.wait()


def tail_kernel(pos_s, xf, kn, vn, ext, ring, skv, logit_h, nk_h, nv_h, lbuf, stage, newt, sem_l, sem_n):
    _, n_layer, n_chunk, _, width, ctx = skv.shape
    n_seq = n_chunk * GROUP
    n_group = n_chunk // PARTS
    n_vocab = lbuf.shape[0]
    ahead = 2 * SLOTS
    model = xf.shape[1]
    split = model - ext.shape[3]
    n_write = 2 * n_layer * n_chunk

    def l_copy(c):
        return pltpu.make_async_copy(lbuf.at[c], logit_h.at[:, pl.ds(c * VOCAB_CHUNK, VOCAB_CHUNK)], sem_l.at[c])

    def n_copy(i):
        kv, layer, c = i // (n_layer * n_chunk), i // n_chunk % n_layer, i % n_chunk
        return pltpu.make_async_copy(stage.at[i % STAGE_SLOTS], (nk_h, nv_h)[kv].at[layer, c // n_group, :, c % n_group], sem_n.at[i % STAGE_SLOTS])

    lane = lax.broadcasted_iota(jnp.int32, (16, ctx), 1)

    def write(i):
        kv, layer, c = i // (n_layer * n_chunk), i // n_chunk % n_layer, i % n_chunk
        if c == 0:
            newt[...] = (kn, vn)[kv][layer].T
        if i >= STAGE_SLOTS:
            n_copy(i - STAGE_SLOTS).wait()
        for s in range(GROUP):
            b = (c // n_group * GROUP + s) * n_group + c % n_group
            here = lane == pos_s[b]
            for r in range(0, width, 16):
                column = jnp.broadcast_to(newt[r:r + 16, b:b + 1], (16, ctx)).astype(BF16)
                stage[i % STAGE_SLOTS, s, r:r + 16, :] = jnp.where(here, column, skv[kv, layer, c, s, r:r + 16, :])
        n_copy(i).start()

    def logit(c):
        kv, slot = chunk_place(c, n_layer * n_chunk)
        if c < ahead:
            lbuf[c] = dot_nt(xf[...], ring[kv, slot, :, :, 0:model].reshape(VOCAB_CHUNK, model))
        else:
            left = ring[kv, slot, :, :, model:model + split].reshape(VOCAB_CHUNK, split)
            right = ext[c - ahead].reshape(VOCAB_CHUNK, model - split)
            lbuf[c] = dot_nt(xf[:, 0:split], left) + dot_nt(xf[:, split:model], right)
        l_copy(c).start()

    for i in range(STAGE_SLOTS // 2):
        write(i)
    for i in range(STAGE_SLOTS // 2, n_write):
        write(i)
        if i % 2 and i // 2 < n_vocab:
            logit(i // 2 - STAGE_SLOTS // 4)
    for c in range(n_write // 2 - STAGE_SLOTS // 4, n_vocab):
        logit(c)
    for c in range(n_vocab):
        l_copy(c).wait()
    for i in range(n_write - STAGE_SLOTS, n_write):
        n_copy(i).wait()


def solution(mesh):
    smem = pl.BlockSpec(memory_space=pltpu.SMEM)
    vmem = pl.BlockSpec(memory_space=pltpu.VMEM)
    hbm = pl.BlockSpec(memory_space=ANY)
    dma = pltpu.SemaphoreType.DMA
    on_chip = lambda z: pltpu.with_memory_space_constraint(z, pltpu.VMEM)

    def local_step(tokens, positions, self_keys, self_vals, cross_keys, cross_vals, embed_table, pos_table, w_qkv, w_cq, in_bias, w_out, out_bias, w_fc1, b_fc1, w_fc2, ln_layers, ln_final):
        n_layer, n_seq, ctx, n_head, head_dim = self_keys.shape
        frames = cross_keys.shape[2]
        width = n_head * head_dim
        model = embed_table.shape[1]
        hidden_units = w_fc1.shape[2]
        vocab_rows = embed_table.shape[0]
        n_vocab = vocab_rows // VOCAB_CHUNK
        n_group = n_seq // (PARTS * GROUP)
        flat = lambda cache: jnp.transpose(cache, (0, 1, 3, 4, 2)).reshape(n_layer, PARTS, GROUP, n_group, width, cache.shape[2])
        sk, sv, ck, cv = flat(self_keys), flat(self_vals), flat(cross_keys), flat(cross_vals)

        picked = pl.pallas_call(
            gather_kernel,
            out_shape=pltpu.VMEM((n_seq, model), BF16),
            in_specs=[smem, hbm],
            out_specs=vmem,
            scratch_shapes=[pltpu.VMEM((n_seq, 16, model), BF16), pltpu.VMEM((n_seq, model), F32), dma((n_seq,))],
            name='gather_rows',
        )(tokens, embed_table)

        wqkv = jnp.transpose(w_qkv, (0, 2, 3, 4, 1)).reshape(n_layer, 3 * width, model)
        wcq = jnp.transpose(w_cq, (0, 2, 3, 1)).reshape(n_layer, width, model)
        wout = w_out.reshape(n_layer, 2, width, model)
        embed_chunks = embed_table.reshape(n_vocab, GROUP, width, model)
        n_inst = n_layer * 3 * PARTS
        n_item = PARTS * n_group
        xf, kn, vn, ext, ring, skv = pl.pallas_call(
            layers_kernel,
            out_shape=(
                pltpu.VMEM((n_seq, model), BF16),
                pltpu.VMEM((n_layer, n_seq, width), F32),
                pltpu.VMEM((n_layer, n_seq, width), F32),
                pltpu.VMEM((n_vocab - 2 * SLOTS, GROUP, width, 128), BF16),
                pltpu.VMEM((2, SLOTS, GROUP, width, frames), BF16),
                pltpu.VMEM((2, n_layer, n_item, GROUP, width, ctx), BF16),
            ),
            in_specs=[smem] + [vmem] * 6 + [hbm] * 11,
            out_specs=(vmem,) * 6,
            scratch_shapes=[
                pltpu.VMEM((n_seq, model), F32), pltpu.VMEM((n_group, GROUP * width), F32),
                pltpu.VMEM((n_seq, ctx), F32), pltpu.VMEM(pos_table.shape, BF16),
                pltpu.VMEM(wqkv.shape, BF16), pltpu.VMEM(wcq.shape, BF16), pltpu.VMEM(wout.shape, BF16),
                pltpu.VMEM(w_fc1.shape, BF16), pltpu.VMEM(w_fc2.shape, BF16),
                pltpu.VMEM((4, n_seq, model), BF16), pltpu.VMEM((n_inst, 4, n_seq // PARTS, model), F32),
                dma((1,)), dma((5, n_layer)), dma((2, n_layer, n_item)), dma((2, SLOTS)), dma((2 * n_vocab - 2 * SLOTS,)), dma((3,)), dma((3,)), dma((n_inst, 3)), dma((n_inst, 3)),
            ],
            compiler_params=pltpu.CompilerParams(collective_id=0, has_side_effects=True, vmem_limit_bytes=15 * MIB),
            name='decoder_layers',
        )(positions, on_chip(picked), jnp.transpose(in_bias, (1, 2, 0, 3)), jnp.transpose(out_bias, (1, 0, 2)), ln_layers, b_fc1, ln_final,
          pos_table, wqkv, wcq, wout, w_fc1, w_fc2, sk, sv, ck, cv, embed_chunks)

        logits, nk, nv = pl.pallas_call(
            tail_kernel,
            out_shape=(
                jax.ShapeDtypeStruct((n_seq, vocab_rows), F32),
                jax.ShapeDtypeStruct(sk.shape, BF16),
                jax.ShapeDtypeStruct(sv.shape, BF16),
            ),
            in_specs=[smem] + [vmem] * 6,
            out_specs=(hbm, hbm, hbm),
            scratch_shapes=[
                pltpu.VMEM((n_vocab, n_seq, VOCAB_CHUNK), F32),
                pltpu.VMEM((STAGE_SLOTS, GROUP, width, ctx), BF16), pltpu.VMEM((width, n_seq), F32),
                dma((n_vocab,)), dma((STAGE_SLOTS,)),
            ],
            compiler_params=pltpu.CompilerParams(vmem_limit_bytes=15 * MIB),
            name='logits_and_caches',
        )(positions, *(on_chip(z) for z in (xf, kn, vn, ext, ring, skv)))
        unflat = lambda cache: jnp.transpose(cache.reshape(n_layer, n_seq, n_head, head_dim, ctx), (0, 1, 4, 2, 3))
        return logits, unflat(nk), unflat(nv)

    batch_spec = P('dp')
    cache_spec = P(None, 'dp', None, 'tp', None)
    in_specs = (batch_spec, batch_spec, cache_spec, cache_spec, cache_spec, cache_spec, P('tp', None), P(None, None), P(None, None, None, 'tp', None), P(None, None, 'tp', None), P(None, None, 'tp', None), P(None, None, 'tp', None, None), P(None, None, None), P(None, None, 'tp'), P(None, 'tp'), P(None, 'tp', None), P(None, None, None, None), P(None, None))
    out_specs = (P('dp', 'tp'), cache_spec, cache_spec)
    return jax.shard_map(local_step, mesh=mesh, in_specs=in_specs, out_specs=out_specs, check_vma=False)
```

```python
import jax
import jax.numpy as jnp
from jax import lax
from jax.experimental import pallas as pl
from jax.experimental.pallas import tpu as pltpu
from jax.sharding import PartitionSpec as P

F32 = jnp.float32
BF16 = jnp.bfloat16
MESH = pl.DeviceIdType.MESH
ANY = pl.ANY

SLOTS = 5
GROUP = 4
PARTS = 2
BLOCK = 2
VOCAB_CHUNK = 768
BATCH = 2
WINDOW = 8
PER_BATCH = 3
MIB = 1024 * 1024


def layer_norm(residual, ln_gain, ln_shift):
    row_mean = jnp.mean(residual, axis=-1, keepdims=True)
    centred = residual - row_mean
    variance = jnp.mean(centred * centred, axis=-1, keepdims=True)
    return (centred * lax.rsqrt(variance + 1e-5) * ln_gain + ln_shift).astype(BF16)


def dot_nn(left, right):
    return lax.dot_general(left, right, (((1,), (0,)), ((), ())), preferred_element_type=F32)


def dot_nt(left, right):
    return lax.dot_general(left, right, (((1,), (1,)), ((), ())), preferred_element_type=F32)


def chunk_place(c, n_items):
    return c % 2, (n_items + c // 2 % SLOTS) % SLOTS


def gather_kernel(tok_s, embed_h, emb_o, ebuf, rows, esem):
    n_seq = rows.shape[0]
    shard_rows = embed_h.shape[0]
    first = lax.axis_index('tp') * shard_rows

    def local_row(b):
        local = tok_s[b] - first
        owned = (local >= 0) & (local < shard_rows)
        return jnp.where(owned, local, 0), owned

    def e_copy(b):
        row, _ = local_row(b)
        base = pl.multiple_of((row // 16) * 16, 16)
        return pltpu.make_async_copy(embed_h.at[pl.ds(base, 16)], ebuf.at[b], esem.at[b])

    for b in range(n_seq):
        e_copy(b).start()
    sub = lax.broadcasted_iota(jnp.int32, (16, embed_h.shape[1]), 0)
    for b in range(n_seq):
        row, owned = local_row(b)
        e_copy(b).wait()
        want = jnp.where(owned, row % 16, -1)
        rows[b:b + 1, :] = jnp.sum(jnp.where(sub == want, ebuf[b].astype(F32), 0.0), axis=0, keepdims=True)
    emb_o[...] = rows[...].astype(BF16)


def layers_kernel(pos_s, picked, inb, outb, lnp, bf1, lnf, ptab_h, wqkv_h, wcq_h, wout_h, w1_h, w2_h, sk_h, sv_h, ck_h, cv_h, embed_h,
                  xo, ext, ring, skv,
                  x, kn, vn, of, hot, newt, ptab, wqkv, wcq, wout, w1, w2, emb, ar, sem_p, sem_w, sem_s, sem_c, sem_v, sem_es, sem_er, sem_as, sem_ar):
    n_layer, n_seq, width = kn.shape
    per_part = n_seq // PARTS
    n_group = per_part // GROUP
    layer_items = PARTS * n_group
    n_items = n_layer * layer_items
    stacked = GROUP * width
    frames = ring.shape[-1]
    ctx = skv.shape[-1]
    me = lax.axis_index('tp')
    peers = [lax.rem(me + d, 4) for d in (1, 2, 3)]

    barrier = pltpu.get_barrier_semaphore()
    for peer in peers:
        pl.semaphore_signal(barrier, inc=1, device_id={'tp': peer}, device_id_type=MESH)

    weights = ((wqkv_h, wqkv), (wcq_h, wcq), (wout_h, wout), (w1_h, w1), (w2_h, w2))

    def w_copy(i, layer):
        return pltpu.make_async_copy(weights[i][0].at[layer], weights[i][1].at[layer], sem_w.at[i, layer])

    def s_copy(kv, layer, item):
        part, g = divmod(item, n_group)
        return pltpu.make_async_copy((sk_h, sv_h)[kv].at[layer, part, :, g], skv.at[kv, layer, item], sem_s.at[kv, layer, item])

    def c_copy(kv, item):
        slot = item % SLOTS
        layer, rest = divmod(item, layer_items)
        part, g = divmod(rest, n_group)
        return pltpu.make_async_copy((ck_h, cv_h)[kv].at[layer, part, :, g], ring.at[kv, slot], sem_c.at[kv, slot])

    def start_self(layer, part):
        for item in range(part * n_group, (part + 1) * n_group):
            s_copy(0, layer, item).start()
            s_copy(1, layer, item).start()

    def start_weights(layer, which):
        for i in which:
            w_copy(i, layer).start()

    ahead = 2 * SLOTS
    n_extra = ext.shape[0]
    model = embed_h.shape[3]
    split = model - ext.shape[3]

    def v_copies(c):
        kv, slot = chunk_place(c, n_items)
        if c < ahead:
            return [pltpu.make_async_copy(embed_h.at[c], ring.at[kv, slot, :, :, pl.ds(0, model)], sem_v.at[c])]
        return [
            pltpu.make_async_copy(embed_h.at[c, :, :, pl.ds(0, split)], ring.at[kv, slot, :, :, pl.ds(model, split)], sem_v.at[c]),
            pltpu.make_async_copy(embed_h.at[c, :, :, pl.ds(split, model - split)], ext.at[c - ahead], sem_v.at[c + n_extra]),
        ]

    def start_cross(items):
        for item in items:
            for kv in range(2):
                if item < n_items:
                    c_copy(kv, item).start()
                else:
                    c = (item - n_items) * 2 + kv
                    for chunk in (c, c + ahead):
                        if chunk < ahead + n_extra:
                            for copy in v_copies(chunk):
                                copy.start()

    tab_copy = pltpu.make_async_copy(ptab_h, ptab, sem_p.at[0])
    tab_copy.start()
    start_weights(0, (0,))
    for part in range(PARTS):
        start_self(0, part)
        start_weights(0, ((2,), (1,))[part])

    pl.semaphore_wait(barrier, 3)
    start_cross((0, 1))

    def e_copy(d):
        return pltpu.make_async_remote_copy(picked, emb.at[me], sem_es.at[d], sem_er.at[d], device_id={'tp': peers[d]}, device_id_type=MESH)

    for d in range(3):
        e_copy(d).start()
    emb[me] = picked[...]
    tab_lane = lax.broadcasted_iota(jnp.int32, (1, ptab.shape[0]), 1)
    for b in range(n_seq):
        hot[b:b + 1, :] = jnp.where(tab_lane == pos_s[b], 1.0, 0.0)
    tab_copy.wait()
    x[...] = dot_nn(hot[...].astype(BF16), ptab[...])
    for d in range(3):
        e_copy(d).wait()
    x[...] = (emb[0].astype(F32) + emb[1].astype(F32) + emb[2].astype(F32) + emb[3].astype(F32)) + x[...]
    start_cross((2, 3, 4))

    lane_block = lax.div(lax.broadcasted_iota(jnp.int32, (16, stacked), 1), 64)
    block_mask = lax.broadcasted_iota(jnp.int32, (16, stacked), 0) == lane_block
    row_seq = lax.div(lax.broadcasted_iota(jnp.int32, (16, 1), 0), width // 64)
    lane = lax.broadcasted_iota(jnp.int32, (16, ctx), 1)

    def a_copy(inst, d):
        return pltpu.make_async_remote_copy(ar.at[inst, me], ar.at[inst, me], sem_as.at[inst, d], sem_ar.at[inst, d], device_id={'tp': peers[d]}, device_id_type=MESH)

    def send(inst, value):
        ar[inst, me] = value
        for d in range(3):
            a_copy(inst, d).start()

    def receive(inst, rows, bias):
        for d in range(3):
            a_copy(inst, d).wait_recv()
        total = (ar[inst, 0] + ar[inst, 1]) + (ar[inst, 2] + ar[inst, 3])
        x[rows, :] = (x[rows, :] + total.astype(BF16).astype(F32)) + bias

    def in_bias_row(kind, layer):
        return jnp.concatenate([inb[kind, h, layer:layer + 1, :] for h in range(3)], axis=1)

    def stack(rows):
        return jnp.concatenate([rows[u * n_group:(u + 1) * n_group] for u in range(GROUP)], axis=1)

    def query_blocks(flat):
        return [jnp.where(block_mask, flat[g:g + 1] * 0.125, 0.0) for g in range(n_group)]

    def fold(mixed):
        return jnp.sum(jnp.where(block_mask, mixed, 0.0), axis=0, keepdims=True)

    def attended():
        return jnp.concatenate([of[:, u * width:(u + 1) * width] for u in range(GROUP)], axis=0).astype(BF16)

    def round32(z):
        return z.astype(BF16).astype(F32)

    def self_stage(layer, part, rows):
        hidden = layer_norm(x[rows, :], lnp[layer, 0, 0:1, :], lnp[layer, 0, 1:2, :])

        if part == 0:
            w_copy(0, layer).wait()
            w_copy(2, layer).wait()

        q = round32(dot_nt(hidden, wqkv[layer, 0:width, :]) + in_bias_row(0, layer))
        k_new = round32(dot_nt(hidden, wqkv[layer, width:2 * width, :]))
        v_new = round32(dot_nt(hidden, wqkv[layer, 2 * width:3 * width, :]) + in_bias_row(1, layer))
        kn[layer, rows, :] = k_new
        vn[layer, rows, :] = v_new
        k_flat, v_flat = stack(k_new), stack(v_new)
        items = [part * n_group + g for g in range(n_group)]
        for item in items:
            s_copy(0, layer, item).wait()
            s_copy(1, layer, item).wait()
        blocks = query_blocks(stack(q))
        scores = [dot_nn(blocks[g].astype(BF16), skv[0, layer, items[g]].reshape(stacked, ctx)) for g in range(n_group)]
        mixed = []
        for g in range(n_group):
            limit = jnp.full((16, 1), 0, jnp.int32)
            for u in range(GROUP):
                limit = jnp.where(row_seq == u, pos_s[part * per_part + u * n_group + g], limit)
            past = lane < limit
            s = jnp.where(past, scores[g], -1e30)
            s_new = jnp.sum(blocks[g] * k_flat[g:g + 1], axis=1, keepdims=True)
            peak = jnp.maximum(jnp.max(s, axis=1, keepdims=True), s_new)
            e = jnp.where(past, jnp.exp(s - peak), 0.0)
            e_new = jnp.exp(s_new - peak)
            inv = 1.0 / (jnp.sum(e, axis=1, keepdims=True) + e_new)
            w_new = round32(e_new * inv)
            mixed.append(dot_nt((e * inv).astype(BF16), skv[1, layer, items[g]].reshape(stacked, ctx)) + w_new * v_flat[g:g + 1])
        for g in range(n_group):
            of[g:g + 1, :] = fold(mixed[g])
        return dot_nn(attended(), wout[layer, 0])

    def cross_stage(layer, part, rows):
        hidden = layer_norm(x[rows, :], lnp[layer, 1, 0:1, :], lnp[layer, 1, 1:2, :])

        if part == 0:
            w_copy(1, layer).wait()

        q = round32(dot_nt(hidden, wcq[layer]) + in_bias_row(2, layer))
        blocks = query_blocks(stack(q))
        items = [(layer * PARTS + part) * n_group + g for g in range(n_group)]
        mixed = []
        for first in range(0, n_group, BLOCK):
            block = range(first, first + BLOCK)
            for g in block:
                c_copy(0, items[g]).wait()
                c_copy(1, items[g]).wait()
            scores = [dot_nn(blocks[g].astype(BF16), ring[0, items[g] % SLOTS].reshape(stacked, frames)) for g in block]
            for g in block:
                s = scores[g - first]
                e = jnp.exp(s - jnp.max(s, axis=1, keepdims=True))
                inv = 1.0 / jnp.sum(e, axis=1, keepdims=True)
                mixed.append(dot_nt((e * inv).astype(BF16), ring[1, items[g] % SLOTS].reshape(stacked, frames)))
            for g in block:
                of[g:g + 1, :] = fold(mixed[g])
            start_cross([items[g] + SLOTS for g in block])
        heads = attended()
        return dot_nn(heads, wout[layer, 1])

    def mlp_stage(layer, part, rows):
        hidden = layer_norm(x[rows, :], lnp[layer, 2, 0:1, :], lnp[layer, 2, 1:2, :])

        if part == 0:
            w_copy(3, layer).wait()
            w_copy(4, layer).wait()

        pre = dot_nn(hidden, w1[layer]) + bf1[layer:layer + 1, :]
        active = (0.5 * pre * (1.0 + lax.erf(pre * (0.5 ** 0.5)))).astype(BF16)
        return dot_nn(active, w2[layer])

    def update(layer, kv):
        newt[...] = (kn, vn)[kv][layer].T
        for item in range(layer_items):
            for u in range(GROUP):
                b = (item // n_group * GROUP + u) * n_group + item % n_group
                here = lane == pos_s[b]
                for r in range(0, width, 16):
                    column = jnp.broadcast_to(newt[r:r + 16, b:b + 1], (16, ctx)).astype(BF16)
                    skv[kv, layer, item, u, r:r + 16, :] = jnp.where(here, column, skv[kv, layer, item, u, r:r + 16, :])

    stages = (self_stage, cross_stage, mlp_stage)
    def start_ahead(layer, kind, part):
        if kind == 0 and layer == 0:
            if part:
                start_weights(0, (3, 4))
        if layer + 1 < n_layer:
            if kind == 1:
                if part == 0:
                    start_weights(layer + 1, (0,))
                start_self(layer + 1, part)
                start_weights(layer + 1, ((2,), (1,))[part])
            if kind == 2 and part == 0:
                start_weights(layer + 1, (3, 4))

    for step in range(n_layer * 3 + 1):
        for part in range(PARTS):
            rows = pl.ds(part * per_part, per_part)
            if step:
                prev_layer, prev_kind = divmod(step - 1, 3)
                receive((step - 1) * PARTS + part, rows, outb[prev_kind, prev_layer:prev_layer + 1, :])
            if step < n_layer * 3:
                layer, kind = divmod(step, 3)
                send(step * PARTS + part, stages[kind](layer, part, rows))
                start_ahead(layer, kind, part)
                if part == PARTS - 1 and kind != 1:
                    update(layer, kind // 2)
    xo[...] = layer_norm(x[...], lnf[0:1, :], lnf[1:2, :])
    for inst in range(n_layer * 3 * PARTS):
        for d in range(3):
            a_copy(inst, d).wait_send()
    for c in range(ahead + n_extra):
        for copy in v_copies(c):
            copy.wait()


def tail_kernel(xf, ext, ring, skv, logit_h, nk_h, nv_h, lbuf, sem_l, sem_n):
    _, n_layer, n_chunk, _, _, _ = skv.shape
    n_group = n_chunk // PARTS
    n_vocab = lbuf.shape[0]
    ahead = 2 * SLOTS
    model = xf.shape[1]
    split = model - ext.shape[3]

    def l_copy(c):
        return pltpu.make_async_copy(lbuf.at[c], logit_h.at[:, pl.ds(c * VOCAB_CHUNK, VOCAB_CHUNK)], sem_l.at[c])

    def n_copies():
        for kv, out_h in enumerate((nk_h, nv_h)):
            for layer in range(n_layer):
                for c in range(n_chunk):
                    yield pltpu.make_async_copy(skv.at[kv, layer, c], out_h.at[layer, c // n_group, :, c % n_group], sem_n.at[kv, layer, c])

    def logit(c):
        kv, slot = chunk_place(c, n_layer * n_chunk)
        if c < ahead:
            lbuf[c] = dot_nt(xf[...], ring[kv, slot, :, :, 0:model].reshape(VOCAB_CHUNK, model))
        else:
            left = ring[kv, slot, :, :, model:model + split].reshape(VOCAB_CHUNK, split)
            right = ext[c - ahead].reshape(VOCAB_CHUNK, model - split)
            lbuf[c] = dot_nt(xf[:, 0:split], left) + dot_nt(xf[:, split:model], right)

    writes = list(n_copies())
    for copy in writes[:WINDOW]:
        copy.start()
    head, tail = 0, WINDOW
    for first in range(0, n_vocab, BATCH):
        batch = range(first, min(first + BATCH, n_vocab))
        for c in batch:
            logit(c)
        for c in batch:
            l_copy(c).start()
        for _ in range(PER_BATCH):
            if tail < len(writes):
                writes[head].wait()
                writes[tail].start()
                head, tail = head + 1, tail + 1
    for c in range(n_vocab):
        l_copy(c).wait()
    for copy in writes[head:]:
        copy.wait()


def solution(mesh):
    smem = pl.BlockSpec(memory_space=pltpu.SMEM)
    vmem = pl.BlockSpec(memory_space=pltpu.VMEM)
    hbm = pl.BlockSpec(memory_space=ANY)
    dma = pltpu.SemaphoreType.DMA
    on_chip = lambda z: pltpu.with_memory_space_constraint(z, pltpu.VMEM)

    def local_step(tokens, positions, self_keys, self_vals, cross_keys, cross_vals, embed_table, pos_table, w_qkv, w_cq, in_bias, w_out, out_bias, w_fc1, b_fc1, w_fc2, ln_layers, ln_final):
        n_layer, n_seq, ctx, n_head, head_dim = self_keys.shape
        frames = cross_keys.shape[2]
        width = n_head * head_dim
        model = embed_table.shape[1]
        hidden_units = w_fc1.shape[2]
        vocab_rows = embed_table.shape[0]
        n_vocab = vocab_rows // VOCAB_CHUNK
        n_group = n_seq // (PARTS * GROUP)
        flat = lambda cache: jnp.transpose(cache, (0, 1, 3, 4, 2)).reshape(n_layer, PARTS, GROUP, n_group, width, cache.shape[2])
        sk, sv, ck, cv = flat(self_keys), flat(self_vals), flat(cross_keys), flat(cross_vals)

        picked = pl.pallas_call(
            gather_kernel,
            out_shape=pltpu.VMEM((n_seq, model), BF16),
            in_specs=[smem, hbm],
            out_specs=vmem,
            scratch_shapes=[pltpu.VMEM((n_seq, 16, model), BF16), pltpu.VMEM((n_seq, model), F32), dma((n_seq,))],
            name='gather_rows',
        )(tokens, embed_table)

        wqkv = jnp.transpose(w_qkv, (0, 2, 3, 4, 1)).reshape(n_layer, 3 * width, model)
        wcq = jnp.transpose(w_cq, (0, 2, 3, 1)).reshape(n_layer, width, model)
        wout = w_out.reshape(n_layer, 2, width, model)
        embed_chunks = embed_table.reshape(n_vocab, GROUP, width, model)
        n_inst = n_layer * 3 * PARTS
        n_item = PARTS * n_group
        xf, ext, ring, skv = pl.pallas_call(
            layers_kernel,
            out_shape=(
                pltpu.VMEM((n_seq, model), BF16),
                pltpu.VMEM((n_vocab - 2 * SLOTS, GROUP, width, 128), BF16),
                pltpu.VMEM((2, SLOTS, GROUP, width, frames), BF16),
                pltpu.VMEM((2, n_layer, n_item, GROUP, width, ctx), BF16),
            ),
            in_specs=[smem] + [vmem] * 6 + [hbm] * 11,
            out_specs=(vmem,) * 4,
            scratch_shapes=[
                pltpu.VMEM((n_seq, model), F32), pltpu.VMEM((n_layer, n_seq, width), F32), pltpu.VMEM((n_layer, n_seq, width), F32),
                pltpu.VMEM((n_group, GROUP * width), F32),
                pltpu.VMEM((n_seq, ctx), F32), pltpu.VMEM((width, n_seq), F32), pltpu.VMEM(pos_table.shape, BF16),
                pltpu.VMEM(wqkv.shape, BF16), pltpu.VMEM(wcq.shape, BF16), pltpu.VMEM(wout.shape, BF16),
                pltpu.VMEM(w_fc1.shape, BF16), pltpu.VMEM(w_fc2.shape, BF16),
                pltpu.VMEM((4, n_seq, model), BF16), pltpu.VMEM((n_inst, 4, n_seq // PARTS, model), F32),
                dma((1,)), dma((5, n_layer)), dma((2, n_layer, n_item)), dma((2, SLOTS)), dma((2 * n_vocab - 2 * SLOTS,)), dma((3,)), dma((3,)), dma((n_inst, 3)), dma((n_inst, 3)),
            ],
            compiler_params=pltpu.CompilerParams(collective_id=0, has_side_effects=True, vmem_limit_bytes=15 * MIB),
            name='decoder_layers',
        )(positions, on_chip(picked), jnp.transpose(in_bias, (1, 2, 0, 3)), jnp.transpose(out_bias, (1, 0, 2)), ln_layers, b_fc1, ln_final,
          pos_table, wqkv, wcq, wout, w_fc1, w_fc2, sk, sv, ck, cv, embed_chunks)

        logits, nk, nv = pl.pallas_call(
            tail_kernel,
            out_shape=(
                jax.ShapeDtypeStruct((n_seq, vocab_rows), F32),
                jax.ShapeDtypeStruct(sk.shape, BF16),
                jax.ShapeDtypeStruct(sv.shape, BF16),
            ),
            in_specs=[vmem] * 4,
            out_specs=(hbm, hbm, hbm),
            scratch_shapes=[
                pltpu.VMEM((n_vocab, n_seq, VOCAB_CHUNK), F32),
                dma((n_vocab,)), dma((2, n_layer, n_item)),
            ],
            compiler_params=pltpu.CompilerParams(vmem_limit_bytes=15 * MIB),
            name='logits_and_caches',
        )(*(on_chip(z) for z in (xf, ext, ring, skv)))
        unflat = lambda cache: jnp.transpose(cache.reshape(n_layer, n_seq, n_head, head_dim, ctx), (0, 1, 4, 2, 3))
        return logits, unflat(nk), unflat(nv)

    batch_spec = P('dp')
    cache_spec = P(None, 'dp', None, 'tp', None)
    in_specs = (batch_spec, batch_spec, cache_spec, cache_spec, cache_spec, cache_spec, P('tp', None), P(None, None), P(None, None, None, 'tp', None), P(None, None, 'tp', None), P(None, None, 'tp', None), P(None, None, 'tp', None, None), P(None, None, None), P(None, None, 'tp'), P(None, 'tp'), P(None, 'tp', None), P(None, None, None, None), P(None, None))
    out_specs = (P('dp', 'tp'), cache_spec, cache_spec)
    return jax.shard_map(local_step, mesh=mesh, in_specs=in_specs, out_specs=out_specs, check_vma=False)
```
